32 devices in a mesh: dp: 2 (over x), tp: 4 (over z), sp: 4 (over y, core).
Axes of the slice: x: 2, y: 2, z: 4, core: 2. Of those that a mesh axis runs over, the one named last changes fastest.
Arguments:
- embeds: bfloat16 [16384, 2304], P(('dp', 'sp')), parts along dimension 0
- positions: int32 [16384], P(('dp', 'sp')), parts along dimension 0
- w_query: bfloat16 [2, 2304, 8, 256], P(None, None, 'tp')
- w_key: bfloat16 [2, 2304, 4, 256], P(None, None, 'tp')
- w_value: bfloat16 [2, 2304, 4, 256], P(None, None, 'tp')
- w_out: bfloat16 [2, 8, 256, 2304], P(None, 'tp')
- w_gate: bfloat16 [2, 2304, 9216], P(None, None, 'tp')
- w_up: bfloat16 [2, 2304, 9216], P(None, None, 'tp')
- w_down: bfloat16 [2, 9216, 2304], P(None, 'tp')
- attn_gain: bfloat16 [2, 2304], replicated
- mlp_gain: bfloat16 [2, 2304], replicated
Outputs:
- output 1: bfloat16 [16384, 2304], P(('dp', 'sp')), parts along dimension 0
- output 2: bfloat16 [2, 16384, 4, 256], P(None, ('dp', 'sp'), 'tp'), parts along dimension 1
- output 3: bfloat16 [2, 16384, 4, 256], P(None, ('dp', 'sp'), 'tp'), parts along dimension 1
There are 2 independent parts. The reference program is written for one: setup_inputs(seed, part) draws one part's arguments, and reference() takes and returns one part's arrays. A program takes and returns all parts, laid end to end along the dimension named above; an argument that names none is the same for every part.
All inputs are finite; a program needn't handle non-finite values.
Results may differ from the reference program's by a relative error of at most 0.02.
Values are sent between devices in bfloat16 or wider.
A program may use at most 1 GiB of HBM per device.

```python
import jax
import jax.numpy as jnp
from jax import lax

SEQ_LEN = 8192
D_MODEL = 2304
NUM_HEADS = 8
KV_HEADS = 4
HEAD_DIM = 256
FFN_DIM = 9216
WINDOW = 1024
LAYERS = 2
QUERY_BLOCK = 32

ROPE_BASE = 10000.0
NORM_EPS = 1e-6


def setup_inputs(seed: int = 0, part: int = 0) -> dict:
    root_key = jax.random.key(seed)
    shared_key, part_root = jax.random.split(root_key)
    part_key = jax.random.fold_in(part_root, part)
    key_embed, key_start, key_step = jax.random.split(part_key, 3)
    weight_keys = jax.random.split(shared_key, 9)
    embeds = jax.random.normal(key_embed, (SEQ_LEN, D_MODEL), jnp.float32).astype(jnp.bfloat16)
    pos_start = jax.random.randint(key_start, (1,), 0, 1024, dtype=jnp.int32)
    pos_steps = jax.random.randint(key_step, (SEQ_LEN,), 1, 3, dtype=jnp.int32)
    positions = pos_start + jnp.cumsum(pos_steps) - pos_steps[0]
    qk_scale = 1.4 * D_MODEL ** -0.5
    in_scale = D_MODEL ** -0.5
    out_scale = 2.0 * (NUM_HEADS * HEAD_DIM) ** -0.5
    down_scale = FFN_DIM ** -0.5

    def normal_weight(key_w, shape_w, scale_w):
        return (jax.random.normal(key_w, shape_w, jnp.float32) * scale_w).astype(jnp.bfloat16)

    def gain_draw(key_w):
        return (1.0 + 0.4 * jax.random.normal(key_w, (LAYERS, D_MODEL), jnp.float32)).astype(jnp.bfloat16)

    return {
        'embeds': embeds,
        'positions': positions,
        'w_query': normal_weight(weight_keys[0], (LAYERS, D_MODEL, NUM_HEADS, HEAD_DIM), qk_scale),
        'w_key': normal_weight(weight_keys[1], (LAYERS, D_MODEL, KV_HEADS, HEAD_DIM), qk_scale),
        'w_value': normal_weight(weight_keys[2], (LAYERS, D_MODEL, KV_HEADS, HEAD_DIM), in_scale),
        'w_out': normal_weight(weight_keys[3], (LAYERS, NUM_HEADS, HEAD_DIM, D_MODEL), out_scale),
        'w_gate': normal_weight(weight_keys[4], (LAYERS, D_MODEL, FFN_DIM), in_scale),
        'w_up': normal_weight(weight_keys[5], (LAYERS, D_MODEL, FFN_DIM), in_scale),
        'w_down': normal_weight(weight_keys[6], (LAYERS, FFN_DIM, D_MODEL), down_scale),
        'attn_gain': gain_draw(weight_keys[7]),
        'mlp_gain': gain_draw(weight_keys[8]),
    }


def rms_norm(hidden, gain_vec):
    hidden_f = hidden.astype(jnp.float32)
    inv_rms = lax.rsqrt(jnp.mean(hidden_f * hidden_f, axis=-1, keepdims=True) + NORM_EPS)
    return (hidden_f * inv_rms * gain_vec.astype(jnp.float32)).astype(jnp.bfloat16)


def rotary(head_vals, positions):
    half_dim = HEAD_DIM // 2
    inv_freq = ROPE_BASE ** (-2.0 * jnp.arange(half_dim, dtype=jnp.float32) / HEAD_DIM)
    angles = positions.astype(jnp.float32)[:, None] * inv_freq[None, :]
    cosine = jnp.cos(angles)[:, None, :]
    sine_val = jnp.sin(angles)[:, None, :]
    heads_f = head_vals.astype(jnp.float32)
    first_half = heads_f[..., :half_dim]
    second_half = heads_f[..., half_dim:]
    rotated = jnp.concatenate([first_half * cosine - second_half * sine_val, second_half * cosine + first_half * sine_val], axis=-1)
    return rotated.astype(jnp.bfloat16)


def attention(queries, keys_rot, values_new, windowed):
    group_size = NUM_HEADS // KV_HEADS
    q_full = queries.reshape(SEQ_LEN, KV_HEADS, group_size, HEAD_DIM).astype(jnp.float32)
    k_full = keys_rot.astype(jnp.float32)
    v_full = values_new.astype(jnp.float32)
    qk_scale = HEAD_DIM ** -0.5
    key_span = WINDOW + QUERY_BLOCK
    if windowed:
        pad_rows = jnp.zeros((WINDOW, KV_HEADS, HEAD_DIM), jnp.float32)
        k_full = jnp.concatenate([pad_rows, k_full], axis=0)
        v_full = jnp.concatenate([pad_rows, v_full], axis=0)

    def one_block(block_id):
        row_start = block_id * QUERY_BLOCK
        q_rows = lax.dynamic_slice_in_dim(q_full, row_start, QUERY_BLOCK, 0)
        q_index = row_start + jnp.arange(QUERY_BLOCK)
        if windowed:
            k_rows = lax.dynamic_slice_in_dim(k_full, row_start, key_span, 0)
            v_rows = lax.dynamic_slice_in_dim(v_full, row_start, key_span, 0)
            k_index = row_start - WINDOW + jnp.arange(key_span)
        else:
            k_rows = k_full
            v_rows = v_full
            k_index = jnp.arange(SEQ_LEN)
        logits = jnp.einsum('tkgd,skd->tkgs', q_rows, k_rows) * qk_scale
        dist_rows = q_index[:, None] - k_index[None, :]
        visible = (dist_rows >= 0) & (k_index[None, :] >= 0)
        if windowed:
            visible = visible & (dist_rows <= WINDOW)
        masked = jnp.where(visible[:, None, None, :], logits, -1e30)
        row_peak = jnp.max(masked, axis=-1, keepdims=True)
        weights = jnp.exp(masked - row_peak)
        probs_bf = (weights / jnp.sum(weights, axis=-1, keepdims=True)).astype(jnp.bfloat16)
        attn_out = jnp.einsum('tkgs,skd->tkgd', probs_bf.astype(jnp.float32), v_rows)
        return attn_out.astype(jnp.bfloat16)

    blocks_out = lax.map(one_block, jnp.arange(SEQ_LEN // QUERY_BLOCK))
    return blocks_out.reshape(SEQ_LEN, NUM_HEADS * HEAD_DIM)


def reference(embeds, positions, w_query, w_key, w_value, w_out, w_gate, w_up, w_down, attn_gain, mlp_gain):
    hidden = embeds
    k_layers = []
    v_layers = []
    for layer_id in range(LAYERS):
        normed = rms_norm(hidden, attn_gain[layer_id])
        queries = jnp.dot(normed, w_query[layer_id].reshape(D_MODEL, NUM_HEADS * HEAD_DIM), preferred_element_type=jnp.float32).astype(jnp.bfloat16).reshape(SEQ_LEN, NUM_HEADS, HEAD_DIM)
        keys_new = jnp.dot(normed, w_key[layer_id].reshape(D_MODEL, KV_HEADS * HEAD_DIM), preferred_element_type=jnp.float32).astype(jnp.bfloat16).reshape(SEQ_LEN, KV_HEADS, HEAD_DIM)
        values_new = jnp.dot(normed, w_value[layer_id].reshape(D_MODEL, KV_HEADS * HEAD_DIM), preferred_element_type=jnp.float32).astype(jnp.bfloat16).reshape(SEQ_LEN, KV_HEADS, HEAD_DIM)
        queries = rotary(queries, positions)
        keys_rot = rotary(keys_new, positions)
        attn_rows = attention(queries, keys_rot, values_new, layer_id % 2 == 0)
        attn_sum = jnp.dot(attn_rows, w_out[layer_id].reshape(NUM_HEADS * HEAD_DIM, D_MODEL), preferred_element_type=jnp.float32).astype(jnp.bfloat16)
        hidden = (hidden.astype(jnp.float32) + attn_sum.astype(jnp.float32)).astype(jnp.bfloat16)
        normed = rms_norm(hidden, mlp_gain[layer_id])
        gate_proj = jnp.dot(normed, w_gate[layer_id], preferred_element_type=jnp.float32)
        up_proj = jnp.dot(normed, w_up[layer_id], preferred_element_type=jnp.float32)
        hidden_act = (jax.nn.silu(gate_proj) * up_proj).astype(jnp.bfloat16)
        mlp_sum = jnp.dot(hidden_act, w_down[layer_id], preferred_element_type=jnp.float32).astype(jnp.bfloat16)
        hidden = (hidden.astype(jnp.float32) + mlp_sum.astype(jnp.float32)).astype(jnp.bfloat16)
        k_layers.append(keys_rot)
        v_layers.append(values_new)
    return hidden, jnp.stack(k_layers), jnp.stack(v_layers)
```

```python
import functools

import jax
import jax.numpy as jnp
from jax import lax
from jax.experimental import pallas as pl
from jax.experimental.pallas import tpu as pltpu
from jax.sharding import PartitionSpec as P


ROPE_BASE = 10000.0
NORM_EPS = 1e-6
WINDOW = 1024
HEAD = 256
HALF = 128
TQ = 512
TW = 256
EXP_SCALE = (HEAD ** -0.5) * 1.4426950408889634
NEG = -1.6e31
F32 = jnp.float32
BF16 = jnp.bfloat16


def rms_norm(hidden, gain_vec):
    hidden_f = hidden.astype(F32)
    inv_rms = lax.rsqrt(jnp.mean(hidden_f * hidden_f, axis=-1, keepdims=True) + NORM_EPS)
    return (hidden_f * inv_rms * gain_vec.astype(F32)).astype(BF16)


def rope_tables(positions):
    inv_freq = ROPE_BASE ** (-2.0 * jnp.arange(HALF, dtype=F32) / HEAD)
    angles = positions.astype(F32)[:, None] * inv_freq[None, :]
    return jnp.cos(angles), jnp.sin(angles)


def rotate(vals, cosine, sine, num_heads):
    parts = []
    for h in range(num_heads):
        a = vals[..., h * HEAD:h * HEAD + HALF].astype(F32)
        b = vals[..., h * HEAD + HALF:(h + 1) * HEAD].astype(F32)
        parts.append((a * cosine - b * sine).astype(BF16))
        parts.append((b * cosine + a * sine).astype(BF16))
    parts.append(vals[..., num_heads * HEAD:])
    return jnp.concatenate(parts, axis=-1)


def dot32(a, b):
    return jnp.dot(a, b, preferred_element_type=F32)


def raw_scores(q, k):
    return lax.dot_general(q, k, (((1,), (1,)), ((), ())), preferred_element_type=F32)


def window_kernel(c_ref, q_ref, kv_ref, o_ref):
    i = pl.program_id(0)
    span = WINDOW + TW
    base = pl.multiple_of(i * TW, TW)
    k = kv_ref[pl.ds(base, span), :HEAD]
    v = kv_ref[pl.ds(base, span), HEAD:]
    row = lax.broadcasted_iota(jnp.int32, (TW, span), 0)
    col = lax.broadcasted_iota(jnp.int32, (TW, span), 1)
    first = jnp.where(c_ref[0] > 0, 0, WINDOW - i * TW)
    visible = (col <= row + WINDOW) & (col >= row) & (col >= first)
    for h in range(2):
        s = raw_scores(q_ref[:, h * HEAD:(h + 1) * HEAD], k)
        s = jnp.where(visible, s, NEG)
        e = jnp.exp2((s - jnp.max(s, axis=-1, keepdims=True)) * EXP_SCALE)
        p = (e / jnp.sum(e, axis=-1, keepdims=True)).astype(BF16)
        o_ref[:, h * HEAD:(h + 1) * HEAD] = dot32(p, v).astype(BF16)


def window_attention(c, q, kv_ext):
    num = q.shape[0]
    return pl.pallas_call(
        window_kernel,
        out_shape=jax.ShapeDtypeStruct((num, 2 * HEAD), BF16),
        grid_spec=pltpu.PrefetchScalarGridSpec(
            num_scalar_prefetch=1,
            grid=(num // TW,),
            in_specs=[
                pl.BlockSpec((TW, 2 * HEAD), lambda i, c: (i, 0)),
                pl.BlockSpec(kv_ext.shape, lambda i, c: (0, 0)),
            ],
            out_specs=pl.BlockSpec((TW, 2 * HEAD), lambda i, c: (i, 0)),
        ),
        compiler_params=pltpu.CompilerParams(vmem_limit_bytes=40 * 2**20),
        cost_estimate=pl.CostEstimate(flops=8 * num * (WINDOW + TW) * HEAD, bytes_accessed=num * HEAD * 14, transcendentals=0),
        name="window_attn",
    )(c, q, kv_ext)


def causal_kernel(c_ref, q_ref, kl_ref, *refs):
    pieces = refs[0:2], refs[2:4], refs[4:6]
    o_ref, m_ref, l_ref, acc_ref, join_ref = refs[6:]
    i = pl.program_id(0)
    num = kl_ref.shape[0]
    c = c_ref[0]
    m_ref[...] = jnp.full(m_ref.shape, NEG, F32)
    l_ref[...] = jnp.zeros(l_ref.shape, F32)
    acc_ref[...] = jnp.zeros(acc_ref.shape, F32)

    @pl.when(i == 0)
    def _():
        for g, (a_ref, b_ref) in enumerate(pieces):
            split = a_ref.shape[0]
            join_ref[g, :split] = a_ref[...]
            join_ref[g, split:] = b_ref[...]

    def block(kv_ref, start, size, diagonal):
        start = pl.multiple_of(start, size)
        k = kv_ref[pl.ds(start, size), :HEAD]
        v = kv_ref[pl.ds(start, size), HEAD:]
        logits = [raw_scores(q_ref[:, h * HEAD:(h + 1) * HEAD], k) for h in range(2)]
        for h in range(2):
            s = logits[h]
            if diagonal:
                row = lax.broadcasted_iota(jnp.int32, s.shape, 0)
                col = lax.broadcasted_iota(jnp.int32, s.shape, 1)
                s = jnp.where(col <= row, s, NEG)
            m_old = m_ref[h]
            m_new = jnp.maximum(m_old, jnp.max(s, axis=-1, keepdims=True))
            scale = jnp.exp2((m_old - m_new) * EXP_SCALE)
            e = jnp.exp2((s - m_new[:, :1]) * EXP_SCALE)
            part = e[:, :HALF]
            for g in range(1, size // HALF):
                part = part + e[:, g * HALF:(g + 1) * HALF]
            l_ref[h] = l_ref[h] * scale + part
            m_ref[h] = m_new
            acc_ref[h] = acc_ref[h] * scale[:, :1] + dot32(e.astype(BF16), v)

    def sweep(kv_ref, lo, hi, size):
        def body(j, carry):
            block(kv_ref, j * size, size, False)
            return carry

        lax.fori_loop(lo, hi, body, 0)

    block(kl_ref, i * TQ, TQ, True)
    sweep(kl_ref, 0, i, TQ)
    for g, seen in enumerate((c % 2 == 1, c >= 2, c >= 2)):
        @pl.when(seen)
        def _(g=g):
            block(join_ref.at[g], 0, num, False)
    for h in range(2):
        total = jnp.sum(l_ref[h], axis=-1, keepdims=True)
        o_ref[:, h * HEAD:(h + 1) * HEAD] = (acc_ref[h] / total).astype(BF16)


def causal_attention(c, q, kvs):
    num = q.shape[0]
    full = [pl.BlockSpec(kv.shape, lambda i, c: (0, 0)) for kv in kvs]
    return pl.pallas_call(
        causal_kernel,
        out_shape=jax.ShapeDtypeStruct((num, 2 * HEAD), BF16),
        grid_spec=pltpu.PrefetchScalarGridSpec(
            num_scalar_prefetch=1,
            grid=(num // TQ,),
            in_specs=[pl.BlockSpec((TQ, 2 * HEAD), lambda i, c: (i, 0))] + full,
            out_specs=pl.BlockSpec((TQ, 2 * HEAD), lambda i, c: (i, 0)),
            scratch_shapes=[
                pltpu.VMEM((2, TQ, HALF), F32),
                pltpu.VMEM((2, TQ, HALF), F32),
                pltpu.VMEM((2, TQ, HEAD), F32),
                pltpu.VMEM((3, num, 2 * HEAD), BF16),
            ],
        ),
        compiler_params=pltpu.CompilerParams(vmem_limit_bytes=56 * 2**20),
        cost_estimate=pl.CostEstimate(flops=8 * num * 4 * num * HEAD, bytes_accessed=num * HEAD * 20, transcendentals=0),
        name="causal_attn",
    )(c, q, *kvs)


def ff_kernel(has_init, h_ref, g_ref, u_ref, d_ref, *rest):
    o_ref = rest[-1]
    n = pl.program_id(0)
    h = h_ref[...]
    g = dot32(h, g_ref[...].reshape(g_ref.shape[-2:]))
    u = dot32(h, u_ref[...].reshape(u_ref.shape[-2:]))
    act = (jax.nn.silu(g) * u).astype(BF16)
    d = d_ref[...].reshape(d_ref.shape[-2:])

    @pl.when(n == 0)
    def _():
        first = dot32(act, d)
        o_ref[...] = rest[0][...] + first if has_init else first

    @pl.when(n > 0)
    def _():
        o_ref[...] += dot32(act, d)


def ff_part(h, weights, init=None):
    g, u, d, layer = weights
    rows, width = h.shape
    if layer is None:
        ff = d.shape[0]
        tn = 384 if ff % 768 else (768 if rows <= 256 else 256)
        shift = ff // tn if u is g else 0
        gate = pl.BlockSpec((width, tn), lambda n: (0, n))
        up = pl.BlockSpec((width, tn), lambda n: (0, n + shift))
        down = pl.BlockSpec((tn, width), lambda n: (n, 0))
    else:
        ff = d.shape[1]
        tn = 768 if rows <= 256 else 256
        gate = up = pl.BlockSpec((1, width, tn), lambda n: (layer, 0, n))
        down = pl.BlockSpec((1, tn, width), lambda n: (layer, n, 0))
    whole = pl.BlockSpec((rows, width), lambda n: (0, 0))
    extra = [] if init is None else [init]
    return pl.pallas_call(
        functools.partial(ff_kernel, init is not None),
        out_shape=jax.ShapeDtypeStruct((rows, width), F32),
        grid=(ff // tn,),
        in_specs=[whole, gate, up, down] + [whole] * len(extra),
        out_specs=whole,
        compiler_params=pltpu.CompilerParams(vmem_limit_bytes=56 * 2**20),
        cost_estimate=pl.CostEstimate(flops=6 * rows * width * ff, bytes_accessed=6 * width * ff, transcendentals=0),
        name="ff_part",
    )(h, g, u, d, *extra)


def solution(mesh):
    num_tp = mesh.shape['tp']
    num_sp = mesh.shape['sp']
    num_plane = mesh.shape['dp'] * num_sp
    row_spec = P(('dp', 'sp'), None)
    pos_spec = P(('dp', 'sp'))
    head_cols = P(None, None, 'tp', None)
    head_rows = P(None, 'tp', None, None)
    ff_cols = P(None, None, 'tp')
    ff_rows = P(None, 'tp', None)
    gain_spec = P(None, None)
    cache_spec = P(None, ('dp', 'sp'), 'tp', None)
    flip = {k: [(i, i ^ k) for i in range(num_tp)] for k in (1, 2, 3)}
    ring_up = [(i, (i + 1) % num_tp) for i in range(num_tp)]
    ring_dn = [(i, (i - 1) % num_tp) for i in range(num_tp)]
    sp_next = [(i, i + 1) for i in range(num_sp - 1)]
    sp_core = [(i, i ^ 1) for i in range(num_sp)]
    sp_far = [(i, i + 2) for i in range(2)]

    def layers(embeds, positions, w_query, w_key, w_value, w_out, w_gate, w_up, w_down, attn_gain, mlp_gain):
        num = embeds.shape[0]
        width = embeds.shape[1]
        own = num // num_tp
        z = lax.axis_index('tp')
        c = lax.axis_index('sp')
        seat = lax.axis_index('dp') * num_sp + c
        c_arr = c.astype(jnp.int32).reshape(1)
        ff = w_gate.shape[2]
        num_layers = w_gate.shape[0]
        heads_w = w_query.shape[2] * HEAD

        def gather_all(w):
            piece = lax.dynamic_index_in_dim(w.reshape(num_plane, -1, w.shape[-1]), seat, 0, keepdims=False)
            return lax.all_gather(piece, ('tp', 'dp', 'sp'), axis=0, tiled=True)

        def plane_gather(piece):
            return lax.all_gather(piece, ('dp', 'sp'), axis=0, tiled=True)

        def ff_pieces(layer_id, splits):
            cols = ff // splits
            rows, drows = width // num_plane, cols // num_plane
            sent = []
            for s in range(splits):
                view = (num_layers, num_plane, rows, ff)
                at = (layer_id, seat, 0, s * cols)
                g = lax.dynamic_slice(w_gate.reshape(view), at, (1, 1, rows, cols)).reshape(rows, cols)
                u = lax.dynamic_slice(w_up.reshape(view), at, (1, 1, rows, cols)).reshape(rows, cols)
                d = lax.dynamic_slice(
                    w_down.reshape(num_layers, splits * num_plane, drows, width),
                    (layer_id, s * num_plane + seat, 0, 0), (1, 1, drows, width)).reshape(drows, width)
                sent += [jnp.concatenate([g, u], axis=1), d]
            return sent

        def cross(piece):
            return lax.ppermute(piece, 'tp', flip[2])

        def qkv_weight(layer_id):
            return jnp.concatenate([
                w_query[layer_id].reshape(width, heads_w),
                w_key[layer_id].reshape(width, HEAD),
                w_value[layer_id].reshape(width, HEAD)], axis=1)

        def place(buf, piece, block):
            return lax.dynamic_update_slice(buf, piece[None], (block,) + (0,) * piece.ndim)

        def spread_heads(attn):
            blocks = attn.reshape(num_tp, own, heads_w)
            buf = jnp.zeros((own, num_tp * heads_w), BF16)
            for k in (2, 3, 1, 0):
                piece = lax.dynamic_index_in_dim(blocks, z ^ k, 0, keepdims=False)
                if k:
                    piece = lax.ppermute(piece, 'tp', flip[k])
                buf = lax.dynamic_update_slice(buf, piece, (0, (z ^ k) * heads_w))
            return buf

        def residual(x, mine, back):
            m = (mine + back).astype(BF16)
            return (x.astype(F32) + m.astype(F32)).astype(BF16)

        def local_ff(layer_id):
            return (w_gate, w_up, w_down, layer_id)

        half = own // 2
        sent0 = []
        for piece in ff_pieces(0, 2):
            sent0.append(cross(piece))
        cosine, sine = rope_tables(positions)

        normed0 = rms_norm(embeds, attn_gain[0])
        weight = qkv_weight(0)
        qkv = dot32(normed0, weight).astype(BF16)
        qkv = rotate(qkv, cosine, sine, 3)
        q0, kv0 = qkv[:, :heads_w], qkv[:, heads_w:]
        halo = lax.ppermute(kv0[num - WINDOW:], 'sp', sp_next)
        kv_ext = jnp.concatenate([halo, kv0], axis=0)
        attn0 = window_attention(c_arr, q0, kv_ext)
        wo0 = gather_all(w_out[0].reshape(heads_w, width))
        gu0 = plane_gather(sent0[0])
        d0 = plane_gather(sent0[1])
        gu1 = plane_gather(sent0[2])
        d1 = plane_gather(sent0[3])
        wo1 = gather_all(w_out[1].reshape(heads_w, width))
        x = lax.dynamic_index_in_dim(embeds.reshape(num_tp, own, width), z, 0, keepdims=False)
        o = dot32(spread_heads(attn0), wo0).astype(BF16)
        x = (x.astype(F32) + o.astype(F32)).astype(BF16)
        h2 = rms_norm(x, mlp_gain[0])
        theirs = lax.ppermute(h2, 'tp', flip[1])
        mine = ff_part(h2, local_ff(0))
        far_gu, far_d = ff_pieces(1, 1)
        far_gu = cross(far_gu)
        first, second = (gu0, gu0, d0, None), (gu1, gu1, d1, None)
        other = ff_part(theirs, local_ff(0))
        other = ff_part(theirs, first, other)
        mine = ff_part(h2, first, mine)
        outs = [ff_part(theirs[:half], second, other[:half])]
        outs.append(ff_part(theirs[half:], second, other[half:]))
        back = [lax.ppermute(out, 'tp', flip[1]) for out in outs]
        mine = ff_part(h2, second, mine)
        gu_far = plane_gather(far_gu)
        x = residual(x, mine, jnp.concatenate(back, axis=0))

        normed = rms_norm(x, attn_gain[1])
        weight = qkv_weight(1)
        cos_half = cosine.reshape(2 * num_tp, half, HALF)
        sin_half = sine.reshape(2 * num_tp, half, HALF)
        qkv1 = jnp.zeros((2 * num_tp, half, heads_w + 2 * HEAD), BF16)

        def project(rows, block):
            pick = functools.partial(lax.dynamic_index_in_dim, index=block, axis=0, keepdims=False)
            return rotate(dot32(rows, weight).astype(BF16), pick(cos_half), pick(sin_half), 3)

        def exchange(pieces):
            kv = jnp.concatenate([p[:, heads_w:] for p in pieces], axis=0)
            core = lax.ppermute(kv, 'sp', sp_core)
            far = lax.ppermute(kv, 'sp', sp_far)
            return core, far

        up, dn = normed[:half], normed[half:]
        done = []
        for s in range(num_tp):
            if s:
                up = lax.ppermute(up, 'tp', ring_up)
                dn = lax.ppermute(dn, 'tp', ring_dn)
            for rows, block in ((up, 2 * lax.rem(z - s + num_tp, num_tp)), (dn, 2 * lax.rem(z + s, num_tp) + 1)):
                out = project(rows, block)
                done.append(out)
                qkv1 = place(qkv1, out, block)
            if s == 2:
                core_a, far_a = exchange(done)
        core_b, far_b = exchange(done[6:])
        diag_a = lax.ppermute(far_a, 'sp', sp_core)
        diag_b = lax.ppermute(far_b, 'sp', sp_core)
        qkv1 = qkv1.reshape(num, heads_w + 2 * HEAD)
        q1, kv1 = qkv1[:, :heads_w], qkv1[:, heads_w:]
        far_d = cross(far_d)
        attn1 = causal_attention(c_arr, q1, (kv1, core_a, core_b, far_a, far_b, diag_a, diag_b))
        d_far = plane_gather(far_d)
        o = dot32(spread_heads(attn1), wo1).astype(BF16)
        x = (x.astype(F32) + o.astype(F32)).astype(BF16)
        h2 = rms_norm(x, mlp_gain[1])
        fetched = (gu_far, gu_far, d_far, None)
        theirs = [lax.ppermute(h2[s * half:(s + 1) * half], 'tp', flip[1]) for s in range(2)]
        out = ff_part(theirs[0], local_ff(1))
        out = ff_part(theirs[0], fetched, out)
        back = [lax.ppermute(out, 'tp', flip[1])]
        out = ff_part(theirs[1], local_ff(1))
        out = ff_part(theirs[1], fetched, out)
        back.append(lax.ppermute(out, 'tp', flip[1]))
        mine = ff_part(h2, fetched, ff_part(h2, local_ff(1)))
        x = residual(x, mine, jnp.concatenate(back, axis=0))

        up, dn = x[:half], x[half:]
        hidden = normed0.reshape(2 * num_tp, half, width)
        hidden = place(place(hidden, up, 2 * z), dn, 2 * z + 1)
        for s in range(1, num_tp):
            up = lax.ppermute(up, 'tp', ring_up)
            dn = lax.ppermute(dn, 'tp', ring_dn)
            hidden = place(hidden, up, 2 * lax.rem(z - s + num_tp, num_tp))
            hidden = place(hidden, dn, 2 * lax.rem(z + s, num_tp) + 1)
        kv = jnp.stack([kv0, kv1])[:, :, None, :]
        return hidden.reshape(num, width), kv[..., :HEAD], kv[..., HEAD:]


    return jax.shard_map(layers, mesh=mesh, in_specs=(row_spec, pos_spec, head_cols, head_cols, head_cols, head_rows, ff_cols, ff_cols, ff_rows, gain_spec, gain_spec), out_specs=(row_spec, cache_spec, cache_spec), check_vma=False)
```

```python
import functools

import jax
import jax.numpy as jnp
from jax import lax
from jax.experimental import pallas as pl
from jax.experimental.pallas import tpu as pltpu
from jax.sharding import PartitionSpec as P


ROPE_BASE = 10000.0
NORM_EPS = 1e-6
WINDOW = 1024
HEAD = 256
HALF = 128
TQ = 512
TW = 256
EXP_SCALE = (HEAD ** -0.5) * 1.4426950408889634
NEG = -1.6e31
F32 = jnp.float32
BF16 = jnp.bfloat16


def rms_norm(hidden, gain_vec):
    hidden_f = hidden.astype(F32)
    inv_rms = lax.rsqrt(jnp.mean(hidden_f * hidden_f, axis=-1, keepdims=True) + NORM_EPS)
    return (hidden_f * inv_rms * gain_vec.astype(F32)).astype(BF16)


def rope_tables(positions):
    inv_freq = ROPE_BASE ** (-2.0 * jnp.arange(HALF, dtype=F32) / HEAD)
    angles = positions.astype(F32)[:, None] * inv_freq[None, :]
    return jnp.cos(angles), jnp.sin(angles)


def rotate(vals, cosine, sine, num_heads):
    parts = []
    for h in range(num_heads):
        a = vals[..., h * HEAD:h * HEAD + HALF].astype(F32)
        b = vals[..., h * HEAD + HALF:(h + 1) * HEAD].astype(F32)
        parts.append((a * cosine - b * sine).astype(BF16))
        parts.append((b * cosine + a * sine).astype(BF16))
    parts.append(vals[..., num_heads * HEAD:])
    return jnp.concatenate(parts, axis=-1)


def dot32(a, b):
    return jnp.dot(a, b, preferred_element_type=F32)


def raw_scores(q, k):
    return lax.dot_general(q, k, (((1,), (1,)), ((), ())), preferred_element_type=F32)


def window_kernel(c_ref, q_ref, kv_ref, o_ref):
    i = pl.program_id(0)
    span = WINDOW + TW
    base = pl.multiple_of(i * TW, TW)
    k = kv_ref[pl.ds(base, span), :HEAD]
    v = kv_ref[pl.ds(base, span), HEAD:]
    row = lax.broadcasted_iota(jnp.int32, (TW, span), 0)
    col = lax.broadcasted_iota(jnp.int32, (TW, span), 1)
    first = jnp.where(c_ref[0] > 0, 0, WINDOW - i * TW)
    visible = (col <= row + WINDOW) & (col >= row) & (col >= first)
    for h in range(2):
        s = raw_scores(q_ref[:, h * HEAD:(h + 1) * HEAD], k)
        s = jnp.where(visible, s, NEG)
        e = jnp.exp2((s - jnp.max(s, axis=-1, keepdims=True)) * EXP_SCALE)
        p = (e / jnp.sum(e, axis=-1, keepdims=True)).astype(BF16)
        o_ref[:, h * HEAD:(h + 1) * HEAD] = dot32(p, v).astype(BF16)


def window_attention(c, q, kv_ext):
    num = q.shape[0]
    return pl.pallas_call(
        window_kernel,
        out_shape=jax.ShapeDtypeStruct((num, 2 * HEAD), BF16),
        grid_spec=pltpu.PrefetchScalarGridSpec(
            num_scalar_prefetch=1,
            grid=(num // TW,),
            in_specs=[
                pl.BlockSpec((TW, 2 * HEAD), lambda i, c: (i, 0)),
                pl.BlockSpec(kv_ext.shape, lambda i, c: (0, 0)),
            ],
            out_specs=pl.BlockSpec((TW, 2 * HEAD), lambda i, c: (i, 0)),
        ),
        compiler_params=pltpu.CompilerParams(vmem_limit_bytes=40 * 2**20),
        cost_estimate=pl.CostEstimate(flops=8 * num * (WINDOW + TW) * HEAD, bytes_accessed=num * HEAD * 14, transcendentals=0),
        name="window_attn",
    )(c, q, kv_ext)


def causal_kernel(c_ref, q_ref, kl_ref, *refs):
    pieces = refs[0:2], refs[2:4], refs[4:6]
    o_ref, m_ref, l_ref, acc_ref, join_ref = refs[6:]
    i = pl.program_id(0)
    num = kl_ref.shape[0]
    c = c_ref[0]
    m_ref[...] = jnp.full(m_ref.shape, NEG, F32)
    l_ref[...] = jnp.zeros(l_ref.shape, F32)
    acc_ref[...] = jnp.zeros(acc_ref.shape, F32)

    @pl.when(i == 0)
    def _():
        for g, (a_ref, b_ref) in enumerate(pieces):
            split = a_ref.shape[0]
            join_ref[g, :split] = a_ref[...]
            join_ref[g, split:] = b_ref[...]

    def block(kv_ref, start, size, diagonal):
        start = pl.multiple_of(start, size)
        k = kv_ref[pl.ds(start, size), :HEAD]
        v = kv_ref[pl.ds(start, size), HEAD:]
        logits = [raw_scores(q_ref[:, h * HEAD:(h + 1) * HEAD], k) for h in range(2)]
        for h in range(2):
            s = logits[h]
            if diagonal:
                row = lax.broadcasted_iota(jnp.int32, s.shape, 0)
                col = lax.broadcasted_iota(jnp.int32, s.shape, 1)
                s = jnp.where(col <= row, s, NEG)
            m_old = m_ref[h]
            m_new = jnp.maximum(m_old, jnp.max(s, axis=-1, keepdims=True))
            scale = jnp.exp2((m_old - m_new) * EXP_SCALE)
            e = jnp.exp2((s - m_new[:, :1]) * EXP_SCALE)
            part = e[:, :HALF]
            for g in range(1, size // HALF):
                part = part + e[:, g * HALF:(g + 1) * HALF]
            l_ref[h] = l_ref[h] * scale + part
            m_ref[h] = m_new
            acc_ref[h] = acc_ref[h] * scale[:, :1] + dot32(e.astype(BF16), v)

    def sweep(kv_ref, lo, hi, size):
        def body(j, carry):
            block(kv_ref, j * size, size, False)
            return carry

        lax.fori_loop(lo, hi, body, 0)

    block(kl_ref, i * TQ, TQ, True)
    sweep(kl_ref, 0, i, TQ)
    for g, seen in enumerate((c % 2 == 1, c >= 2, c >= 2)):
        @pl.when(seen)
        def _(g=g):
            block(join_ref.at[g], 0, num, False)
    for h in range(2):
        total = jnp.sum(l_ref[h], axis=-1, keepdims=True)
        o_ref[:, h * HEAD:(h + 1) * HEAD] = (acc_ref[h] / total).astype(BF16)


def causal_attention(c, q, kvs):
    num = q.shape[0]
    full = [pl.BlockSpec(kv.shape, lambda i, c: (0, 0)) for kv in kvs]
    return pl.pallas_call(
        causal_kernel,
        out_shape=jax.ShapeDtypeStruct((num, 2 * HEAD), BF16),
        grid_spec=pltpu.PrefetchScalarGridSpec(
            num_scalar_prefetch=1,
            grid=(num // TQ,),
            in_specs=[pl.BlockSpec((TQ, 2 * HEAD), lambda i, c: (i, 0))] + full,
            out_specs=pl.BlockSpec((TQ, 2 * HEAD), lambda i, c: (i, 0)),
            scratch_shapes=[
                pltpu.VMEM((2, TQ, HALF), F32),
                pltpu.VMEM((2, TQ, HALF), F32),
                pltpu.VMEM((2, TQ, HEAD), F32),
                pltpu.VMEM((3, num, 2 * HEAD), BF16),
            ],
        ),
        compiler_params=pltpu.CompilerParams(vmem_limit_bytes=56 * 2**20),
        cost_estimate=pl.CostEstimate(flops=8 * num * 4 * num * HEAD, bytes_accessed=num * HEAD * 20, transcendentals=0),
        name="causal_attn",
    )(c, q, *kvs)


def ff_kernel(has_init, h_ref, g_ref, u_ref, d_ref, *rest):
    o_ref = rest[-1]
    n = pl.program_id(0)
    h = h_ref[...]
    g = dot32(h, g_ref[...].reshape(g_ref.shape[-2:]))
    u = dot32(h, u_ref[...].reshape(u_ref.shape[-2:]))
    act = (jax.nn.silu(g) * u).astype(BF16)
    d = d_ref[...].reshape(d_ref.shape[-2:])

    @pl.when(n == 0)
    def _():
        first = dot32(act, d)
        o_ref[...] = rest[0][...] + first if has_init else first

    @pl.when(n > 0)
    def _():
        o_ref[...] += dot32(act, d)


def ff_part(h, weights, init=None):
    g, u, d, layer = weights
    rows, width = h.shape
    if layer is None:
        ff = d.shape[0]
        tn = 384 if ff % 768 else (768 if rows <= 256 else 256)
        shift = ff // tn if u is g else 0
        gate = pl.BlockSpec((width, tn), lambda n: (0, n))
        up = pl.BlockSpec((width, tn), lambda n: (0, n + shift))
        down = pl.BlockSpec((tn, width), lambda n: (n, 0))
    else:
        ff = d.shape[1]
        tn = 768 if rows <= 256 else 256
        gate = up = pl.BlockSpec((1, width, tn), lambda n: (layer, 0, n))
        down = pl.BlockSpec((1, tn, width), lambda n: (layer, n, 0))
    whole = pl.BlockSpec((rows, width), lambda n: (0, 0))
    extra = [] if init is None else [init]
    return pl.pallas_call(
        functools.partial(ff_kernel, init is not None),
        out_shape=jax.ShapeDtypeStruct((rows, width), F32),
        grid=(ff // tn,),
        in_specs=[whole, gate, up, down] + [whole] * len(extra),
        out_specs=whole,
        compiler_params=pltpu.CompilerParams(vmem_limit_bytes=56 * 2**20),
        cost_estimate=pl.CostEstimate(flops=6 * rows * width * ff, bytes_accessed=6 * width * ff, transcendentals=0),
        name="ff_part",
    )(h, g, u, d, *extra)


def solution(mesh):
    num_tp = mesh.shape['tp']
    num_sp = mesh.shape['sp']
    num_plane = mesh.shape['dp'] * num_sp
    row_spec = P(('dp', 'sp'), None)
    pos_spec = P(('dp', 'sp'))
    head_cols = P(None, None, 'tp', None)
    head_rows = P(None, 'tp', None, None)
    ff_cols = P(None, None, 'tp')
    ff_rows = P(None, 'tp', None)
    gain_spec = P(None, None)
    cache_spec = P(None, ('dp', 'sp'), 'tp', None)
    flip = {k: [(i, i ^ k) for i in range(num_tp)] for k in (1, 2, 3)}
    ring_up = [(i, (i + 1) % num_tp) for i in range(num_tp)]
    ring_dn = [(i, (i - 1) % num_tp) for i in range(num_tp)]
    sp_next = [(i, i + 1) for i in range(num_sp - 1)]
    sp_core = [(i, i ^ 1) for i in range(num_sp)]
    sp_far = [(i, i + 2) for i in range(2)]

    def layers(embeds, positions, w_query, w_key, w_value, w_out, w_gate, w_up, w_down, attn_gain, mlp_gain):
        num = embeds.shape[0]
        width = embeds.shape[1]
        own = num // num_tp
        z = lax.axis_index('tp')
        c = lax.axis_index('sp')
        seat = lax.axis_index('dp') * num_sp + c
        c_arr = c.astype(jnp.int32).reshape(1)
        ff = w_gate.shape[2]
        num_layers = w_gate.shape[0]
        heads_w = w_query.shape[2] * HEAD

        def gather_all(w):
            piece = lax.dynamic_index_in_dim(w.reshape(num_plane, -1, w.shape[-1]), seat, 0, keepdims=False)
            return lax.all_gather(piece, ('tp', 'dp', 'sp'), axis=0, tiled=True)

        def plane_gather(piece):
            return lax.all_gather(piece, ('dp', 'sp'), axis=0, tiled=True)

        def ff_pieces(layer_id, splits):
            cols = ff // splits
            rows, drows = width // num_plane, cols // num_plane
            sent = []
            for s in range(splits):
                view = (num_layers, num_plane, rows, ff)
                at = (layer_id, seat, 0, s * cols)
                g = lax.dynamic_slice(w_gate.reshape(view), at, (1, 1, rows, cols)).reshape(rows, cols)
                u = lax.dynamic_slice(w_up.reshape(view), at, (1, 1, rows, cols)).reshape(rows, cols)
                d = lax.dynamic_slice(
                    w_down.reshape(num_layers, splits * num_plane, drows, width),
                    (layer_id, s * num_plane + seat, 0, 0), (1, 1, drows, width)).reshape(drows, width)
                sent += [jnp.concatenate([g, u], axis=1), d]
            return sent

        def cross(piece):
            return lax.ppermute(piece, 'tp', flip[2])

        def qkv_weight(layer_id):
            return jnp.concatenate([
                w_query[layer_id].reshape(width, heads_w),
                w_key[layer_id].reshape(width, HEAD),
                w_value[layer_id].reshape(width, HEAD)], axis=1)

        def place(buf, piece, block):
            return lax.dynamic_update_slice(buf, piece[None], (block,) + (0,) * piece.ndim)

        def spread_heads(attn):
            blocks = attn.reshape(num_tp, own, heads_w)
            buf = jnp.zeros((own, num_tp * heads_w), BF16)
            for k in (2, 3, 1, 0):
                piece = lax.dynamic_index_in_dim(blocks, z ^ k, 0, keepdims=False)
                if k:
                    piece = lax.ppermute(piece, 'tp', flip[k])
                buf = lax.dynamic_update_slice(buf, piece, (0, (z ^ k) * heads_w))
            return buf

        def residual(x, mine, back):
            m = (mine + back).astype(BF16)
            return (x.astype(F32) + m.astype(F32)).astype(BF16)

        def local_ff(layer_id):
            return (w_gate, w_up, w_down, layer_id)

        half = own // 2
        sent0 = []
        for piece in ff_pieces(0, 2):
            sent0.append(cross(piece))
        cosine, sine = rope_tables(positions)

        normed0 = rms_norm(embeds, attn_gain[0])
        weight = qkv_weight(0)
        qkv = dot32(normed0, weight).astype(BF16)
        qkv = rotate(qkv, cosine, sine, 3)
        q0, kv0 = qkv[:, :heads_w], qkv[:, heads_w:]
        halo = lax.ppermute(kv0[num - WINDOW:], 'sp', sp_next)
        kv_ext = jnp.concatenate([halo, kv0], axis=0)
        attn0 = window_attention(c_arr, q0, kv_ext)
        wo0 = gather_all(w_out[0].reshape(heads_w, width))
        gu0 = plane_gather(sent0[0])
        d0 = plane_gather(sent0[1])
        gu1 = plane_gather(sent0[2])
        d1 = plane_gather(sent0[3])
        wo1 = gather_all(w_out[1].reshape(heads_w, width))
        x = lax.dynamic_index_in_dim(embeds.reshape(num_tp, own, width), z, 0, keepdims=False)
        o = dot32(spread_heads(attn0), wo0).astype(BF16)
        x = (x.astype(F32) + o.astype(F32)).astype(BF16)
        h2 = rms_norm(x, mlp_gain[0])
        theirs = lax.ppermute(h2, 'tp', flip[1])
        mine = ff_part(h2, local_ff(0))
        far_gu, far_d = ff_pieces(1, 1)
        far_gu = cross(far_gu)
        first, second = (gu0, gu0, d0, None), (gu1, gu1, d1, None)
        other = ff_part(theirs, local_ff(0))
        other = ff_part(theirs, first, other)
        mine = ff_part(h2, first, mine)
        outs = [ff_part(theirs[:half], second, other[:half])]
        outs.append(ff_part(theirs[half:], second, other[half:]))
        back = [lax.ppermute(out, 'tp', flip[1]) for out in outs]
        mine = ff_part(h2, second, mine)
        gu_far = plane_gather(far_gu)
        x = residual(x, mine, jnp.concatenate(back, axis=0))

        normed = rms_norm(x, attn_gain[1])
        weight = qkv_weight(1)
        cos_half = cosine.reshape(2 * num_tp, half, HALF)
        sin_half = sine.reshape(2 * num_tp, half, HALF)
        qkv1 = jnp.zeros((2 * num_tp, half, heads_w + 2 * HEAD), BF16)

        def project(rows, weight, block):
            pick = functools.partial(lax.dynamic_index_in_dim, index=block, axis=0, keepdims=False)
            out = dot32(rows, weight).astype(BF16)
            return rotate(out, pick(cos_half), pick(sin_half), 3)

        def exchange(kv):
            core = lax.ppermute(kv, 'sp', sp_core)
            far = lax.ppermute(kv, 'sp', sp_far)
            return core, far

        up, dn = normed[:half], normed[half:]
        done = []
        for s in range(num_tp):
            if s:
                up = lax.ppermute(up, 'tp', ring_up)
                dn = lax.ppermute(dn, 'tp', ring_dn)
            for rows, block in ((up, 2 * lax.rem(z - s + num_tp, num_tp)), (dn, 2 * lax.rem(z + s, num_tp) + 1)):
                out = project(rows, weight, block)
                done.append(out)
                qkv1 = place(qkv1, out, block)
            if s == 2:
                kv_a = jnp.concatenate([p[:, heads_w:] for p in done], axis=0)
                kv_a, weight = lax.optimization_barrier((kv_a, weight))
                core_a, far_a = exchange(kv_a)
        core_b, far_b = exchange(jnp.concatenate([p[:, heads_w:] for p in done[6:]], axis=0))
        diag_a = lax.ppermute(far_a, 'sp', sp_core)
        diag_b = lax.ppermute(far_b, 'sp', sp_core)
        qkv1 = qkv1.reshape(num, heads_w + 2 * HEAD)
        q1, kv1 = qkv1[:, :heads_w], qkv1[:, heads_w:]
        far_d = cross(far_d)
        attn1 = causal_attention(c_arr, q1, (kv1, core_a, core_b, far_a, far_b, diag_a, diag_b))
        d_far = plane_gather(far_d)
        o = dot32(spread_heads(attn1), wo1).astype(BF16)
        x = (x.astype(F32) + o.astype(F32)).astype(BF16)
        h2 = rms_norm(x, mlp_gain[1])
        fetched = (gu_far, gu_far, d_far, None)
        theirs = [lax.ppermute(h2[s * half:(s + 1) * half], 'tp', flip[1]) for s in range(2)]
        out = ff_part(theirs[0], local_ff(1))
        out = ff_part(theirs[0], fetched, out)
        back = [lax.ppermute(out, 'tp', flip[1])]
        out = ff_part(theirs[1], local_ff(1))
        out = ff_part(theirs[1], fetched, out)
        back.append(lax.ppermute(out, 'tp', flip[1]))
        mine = ff_part(h2, fetched, ff_part(h2, local_ff(1)))
        x = residual(x, mine, jnp.concatenate(back, axis=0))

        up, dn = x[:half], x[half:]
        hidden = normed0.reshape(2 * num_tp, half, width)
        hidden = place(place(hidden, up, 2 * z), dn, 2 * z + 1)
        for s in range(1, num_tp):
            up = lax.ppermute(up, 'tp', ring_up)
            dn = lax.ppermute(dn, 'tp', ring_dn)
            hidden = place(hidden, up, 2 * lax.rem(z - s + num_tp, num_tp))
            hidden = place(hidden, dn, 2 * lax.rem(z + s, num_tp) + 1)
        kv = jnp.stack([kv0, kv1])[:, :, None, :]
        return hidden.reshape(num, width), kv[..., :HEAD], kv[..., HEAD:]


    return jax.shard_map(layers, mesh=mesh, in_specs=(row_spec, pos_spec, head_cols, head_cols, head_cols, head_rows, ff_cols, ff_cols, ff_rows, gain_spec, gain_spec), out_specs=(row_spec, cache_spec, cache_spec), check_vma=False)
```
